32 devices in a mesh: row: 4 (over y, x), rhs: 8 (over z, core).
Axes of the slice: x: 2, y: 2, z: 4, core: 2. Of those that a mesh axis runs over, the one named last changes fastest.
Arguments:
- factor: float32 [3072, 12, 256], P('row', None, 'rhs'), as said below
- inverses: float32 [12, 256, 256], P('row'), as said below
- right_side: float32 [3072, 4096], P('row', 'rhs'), may hold values from -6 to 6
Outputs:
- solution: float32 [3072, 4096], P('row', 'rhs')
The draws below stay inside these ranges and needn't reach their ends.
Inputs may be any that keep to these rules, and one draw needn't show every extreme that they name: factor[i, j, c] is zero unless j is less than i // 256. Each inverses[p] is lower triangular with a positive diagonal.
All inputs are finite; a program needn't handle non-finite values.
Results may differ from the reference program's by a relative error of at most 0.0001.
Values sent between devices are 32-bit elements; how exact they have to be, the bound alone decides.
No kernel may reach another device: no remote copies, remote signals or barrier semaphores. Data moves between devices by JAX's collectives and lax.ppermute only.
A program may use at most 128 MiB of HBM per device.

```python
import jax
import jax.numpy as jnp
from jax import lax

PANEL = 256
WIN = 3072
NP = 12
NRHS = 4096


def draw_factor(key, part):
    rows = jnp.arange(WIN, dtype=jnp.int32) // PANEL
    cols = jnp.arange(NP, dtype=jnp.int32)
    keep = (cols[None, :] < rows[:, None]).astype(jnp.float32)
    start = jnp.maximum(rows * PANEL, 1).astype(jnp.float32)
    values = jax.random.normal(key, (WIN, NP, PANEL), jnp.float32)
    scales = 0.5
    return values * scales * keep[:, :, None] / jnp.sqrt(start)[:, None, None]


def draw_inverses(key, part):
    lower = jnp.tril(jnp.ones((PANEL, PANEL), jnp.float32), -1)
    values = jax.random.normal(key, (NP, PANEL, PANEL), jnp.float32)
    diag = jax.random.uniform(jax.random.fold_in(key, 3), (NP, PANEL), jnp.float32, 0.6, 1.4)
    return values * lower[None] * (0.5 / jnp.sqrt(PANEL * 1.0)) + diag[:, :, None] * jnp.eye(PANEL, dtype=jnp.float32)[None]


def shard_levels(own_key, extent, cuts, least, top_value):
    loudness = 1.0
    for position, parts in cuts:
        steps = jax.random.uniform(jax.random.fold_in(jax.random.fold_in(own_key, 6), position), (parts,), jnp.float32, least / len(cuts), top_value / len(cuts))
        loudness = loudness * jnp.repeat(jnp.exp(steps), extent[position] // parts).reshape((-1,) + (1,) * (len(extent) - 1 - position))
    return loudness


def bell_draw(key, extent, scale, most, split=(), kind=jnp.bfloat16):
    array = scale * jax.random.normal(key, extent, jnp.float32)
    if split:
        array = array * shard_levels(key, extent, split, -0.22, 0.18)
    return jnp.clip(array, -most, most).astype(kind)


def setup_inputs(seed: int = 0) -> dict:
    key_of = jax.random.split(jax.random.key(seed), 4)
    factor = draw_factor(jax.random.fold_in(key_of[3], 71), 0)
    inverses = draw_inverses(jax.random.fold_in(key_of[3], 71), 0)
    right_side = bell_draw(key_of[2], (WIN, NRHS), 1.0, 6.0, ((0, 4), (1, 8)), jnp.float32)
    return {"factor": factor, "inverses": inverses, "right_side": right_side}


def mult(left, right):
    return jnp.dot(left, right, preferred_element_type=jnp.float32, precision=lax.Precision.HIGHEST)


def reference(factor, inverses, right_side):
    residual = right_side
    pieces = []
    for step in range(NP):
        solved = mult(inverses[step], residual[:PANEL])
        pieces.append(solved)
        residual = residual[PANEL:] - mult(factor[(step + 1) * PANEL:, step, :], solved)
    return jnp.concatenate(pieces, axis=0)
```

```python
import functools

import jax
import jax.numpy as jnp
from jax import lax
from jax.experimental import pallas as pl
from jax.experimental.pallas import tpu as pltpu
from jax.sharding import PartitionSpec as P


CHUNKS = 8
LAG = 2


def halves(value):
    high = value.astype(jnp.bfloat16)
    low = (value - high.astype(jnp.float32)).astype(jnp.bfloat16)
    return high, low


def times(left, high, low, contract=0):
    dims = (((1,), (contract,)), ((), ()))
    left_high, left_low = halves(left)
    dot = functools.partial(lax.dot_general, dimension_numbers=dims, preferred_element_type=jnp.float32)
    return dot(left_high, high) + (dot(left_low, high) + dot(left_high, low))


def prepare_kernel(place, *refs):
    *parts, swapped, high, low = refs
    total = len(parts) * 2
    width = swapped.shape[2]
    for step, part in enumerate(parts):
        source = (place[0] - 2 * step + total) % total
        other = source + 1 - 2 * (source % 2)
        for spot, value in ((source, part[...]), (other, swapped[step])):
            first, second = halves(value)
            spot = pl.multiple_of(spot * width, width)
            high[:, pl.ds(spot, width), :] = first
            low[:, pl.ds(spot, width), :] = second


def split_kernel(value, high, low):
    high[...], low[...] = halves(value[...])


def slot_kernel(slot, lag, chunks, place, residual, inv_high, inv_low, *refs):
    *inputs, out = refs
    count, panel, _ = inv_high.shape
    arrived = inputs[: len(inputs) // 3]
    pairs = inputs[len(inputs) // 3 :]
    row = place[0]
    chunk = slot - lag * row
    rows = out.shape[0]
    valid = jnp.logical_and(chunk >= 0, chunk < chunks)

    @pl.when(jnp.logical_not(valid))
    def _():
        out[...] = jnp.zeros_like(out)

    @pl.when(valid)
    def _():
        out[...] = residual[pl.ds(pl.multiple_of(chunk * rows, rows), rows), :]
        for distance in range(len(arrived), 0, -1):

            @pl.when(row >= distance)
            def _():
                solved = arrived[distance - 1][...]
                out[...] -= times(solved, pairs[2 * distance][...], pairs[2 * distance + 1][...])

        for p in range(count):
            here = slice(p * panel, (p + 1) * panel)
            solved = times(out[:, here], inv_high[p], inv_low[p], 1)
            out[:, here] = solved
            if p + 1 < count:
                rest = slice((p + 1) * panel, count * panel)
                out[:, rest] -= times(solved, pairs[0][here, rest], pairs[1][here, rest])


def whole():
    return pl.BlockSpec(memory_space=pltpu.VMEM)


def body(factor, inverses, right_side):
    block, columns = right_side.shape
    per_block, panel, _ = inverses.shape
    rows = lax.axis_size("row")
    lanes = lax.axis_size("rhs")
    row = lax.axis_index("row")
    lane = lax.axis_index("rhs")
    slices = jnp.transpose(factor, (1, 2, 0))
    width = slices.shape[1]
    piece_rows = columns // CHUNKS
    scalar = pl.BlockSpec(memory_space=pltpu.SMEM)
    place_lane = lane.astype(jnp.int32).reshape(1)
    place_row = row.astype(jnp.int32).reshape(1)

    def send(value, moves):
        pairs = [(a * lanes + b, c * lanes + d) for (a, b), (c, d) in moves]
        return lax.ppermute(value, ("row", "rhs"), pairs)

    residual = jnp.transpose(right_side)
    half = jax.ShapeDtypeStruct
    inv_high, inv_low = pl.pallas_call(
        split_kernel, out_shape=[half(inverses.shape, jnp.bfloat16)] * 2, name="split"
    )(inverses)

    pairs = []
    for distance in range(rows):
        first = jnp.maximum(row - distance, 0) * per_block
        own = lax.dynamic_slice_in_dim(slices, first, per_block, 0)
        users = range(distance, rows)
        parts = [own]
        for step in range(1, lanes // 2):
            parts.append(send(own, [((r, q), (r, (q + 2 * step) % lanes)) for r in users for q in range(lanes)]))
        stacked = jnp.stack(parts)
        swapped = send(stacked, [((r, q), (r, q ^ 1)) for r in users for q in range(lanes)])
        high, low = pl.pallas_call(
            prepare_kernel,
            out_shape=[half((per_block, width * lanes, block), jnp.bfloat16)] * 2,
            in_specs=[scalar] + [whole()] * (len(parts) + 1),
            name="prepare",
        )(place_lane, *parts, swapped)
        pairs += [high.reshape(-1, block), low.reshape(-1, block)]

    slots = CHUNKS + LAG * (rows - 1)
    arrivals = {}
    outs = []
    empty = jnp.zeros((piece_rows, block), jnp.float32)
    for slot in range(slots):
        arrived = [arrivals.get((slot - LAG * d, d), empty) for d in range(1, rows)]
        solved = pl.pallas_call(
            functools.partial(slot_kernel, slot, LAG, CHUNKS),
            out_shape=half((piece_rows, block), jnp.float32),
            in_specs=[scalar] + [whole()] * (3 + len(arrived) + len(pairs)),
            name="slot",
        )(place_row, residual, inv_high, inv_low, *arrived, *pairs)
        outs.append(solved)
        for d in range(1, rows):
            sources = [r for r in range(rows - d) if 0 <= slot - LAG * r < CHUNKS]
            if sources:
                arrivals[slot, d] = send(solved, [((r, q), (r + d, q)) for r in sources for q in range(lanes)])
    stacked = jnp.stack(outs)
    mine = lax.dynamic_slice_in_dim(stacked, row * LAG, CHUNKS, 0)
    return jnp.transpose(mine.reshape(columns, block))


def solution(mesh):
    placed = (P("row", None, "rhs"), P("row", None, None), P("row", "rhs"))
    return jax.shard_map(
        body, mesh=mesh, in_specs=placed, out_specs=P("row", "rhs"), check_vma=False
    )
```

```python
import functools

import jax
import jax.numpy as jnp
from jax import lax
from jax.experimental import pallas as pl
from jax.experimental.pallas import tpu as pltpu
from jax.sharding import PartitionSpec as P


CHUNKS = 4
LAG = 2
GRANT = 20 * 1024 * 1024


def halves(value):
    high = value.astype(jnp.bfloat16)
    low = (value - high.astype(jnp.float32)).astype(jnp.bfloat16)
    return high, low


def times(left, high, low, contract=0):
    dims = (((1,), (contract,)), ((), ()))
    left_high, left_low = halves(left)
    dot = functools.partial(lax.dot_general, dimension_numbers=dims, preferred_element_type=jnp.float32)
    return dot(left_high, high) + (dot(left_low, high) + dot(left_high, low))


def prepare_kernel(masks, place, *refs):
    *parts, swapped, high, low = refs
    width = swapped.shape[2]
    for step, (mask, part) in enumerate(zip(masks, parts)):
        source = place[0] ^ mask
        for spot, value in ((source, part[...]), (source ^ 1, swapped[step])):
            first, second = halves(value)
            spot = pl.multiple_of(spot * width, width)
            high[:, pl.ds(spot, width), :] = first
            low[:, pl.ds(spot, width), :] = second


def turn_kernel(value, out):
    out[...] = value[...].T


def split_kernel(value, high, low):
    high[...], low[...] = halves(value[...])


def solve_into(out, inv_high, inv_low, low_high, low_low):
    count, panel, _ = inv_high.shape
    for p in range(count):
        here = slice(p * panel, (p + 1) * panel)
        solved = times(out[:, here], inv_high[p], inv_low[p], 1)
        out[:, here] = solved
        if p + 1 < count:
            rest = slice((p + 1) * panel, count * panel)
            tiles = (here, slice(p * panel, (count - 1) * panel))
            out[:, rest] -= times(solved, low_high[tiles], low_low[tiles])


def solve_kernel(layout, place, residual, *refs):
    *inputs, out = refs
    names, jobs, finish = layout
    at = dict(zip(names, inputs))
    rows = out.shape[0]
    for row, first, base, terms in jobs:

        @pl.when(place[0] == row)
        def _():
            out[...] = residual[first : first + rows, :] if base is None else at[base][...]
            for spot, key, offset, length, pair in terms:
                here = slice(spot, spot + length)
                solved = at[key][offset : offset + length, :]
                out[here, :] -= times(solved, at[pair + ("high",)][...], at[pair + ("low",)][...])
            if finish:
                solve_into(out, at["inv_high"], at["inv_low"], at["own", "high"], at["own", "low"])


def stack_kernel(*refs):
    *inputs, out = refs
    for step, value in enumerate(inputs):
        out[step] = value[...]


def join_kernel(*refs):
    *inputs, out = refs
    rows = inputs[0].shape[0]
    for step, value in enumerate(inputs):
        out[step * rows : (step + 1) * rows, :] = value[...]


def place_kernel(names, segments, place, *refs):
    *inputs, out, stage, sems = refs
    at = dict(zip(names, inputs))
    for row, parts in enumerate(segments):

        @pl.when(place[0] == row)
        def _():
            copies = []
            for step, (first, length, key) in enumerate(parts):
                copies.append(pltpu.make_async_copy(at[key], stage.at[pl.ds(first, length)], sems.at[step]))
                copies[-1].start()
            for copy in copies:
                copy.wait()

    out[...] = stage[...].T


class Plan:
    def __init__(self, rows, lanes):
        self.rows, self.lanes, self.last = rows, lanes, rows - 1
        self.steps = []
        self.arrived = {}
        self.solved = {row: [] for row in range(rows)}
        if rows == 4:
            self.four()
        else:
            self.many()

    def add(self, *step):
        if step not in self.steps:
            self.steps.append(step)
        return step

    def reach(self, name, *levels):
        count = self.lanes.bit_length() - 2
        for level in levels or range(count):
            bit = self.lanes >> (level + 1)
            for index in range(1 << level):
                self.add("z", name, bit, index)

    def pack(self, name):
        for kind in ("stack", "swap", "prepare"):
            self.add(kind, name)

    def solve(self, *units, base=None, done=(), only=None):
        jobs = []
        for row, first, count in units:
            owners = range(row) if only is None else only
            terms = []
            for owner in owners:
                if owner in done:
                    continue
                chunk = first
                while chunk < first + count:
                    key, start, length = self.arrived[row, owner, chunk]
                    length = min(length - (chunk - start), first + count - chunk)
                    terms.append((chunk - first, key, chunk - start, length, row - owner))
                    chunk += length
            jobs.append((row, first, tuple(terms)))
        key = self.add("solve", units[0][2], tuple(jobs), base, only is None)
        if only is None:
            for row, first, count in units:
                self.solved[row].append((first, count, key))
        return key

    def join(self, *keys):
        return self.add("join", *keys)

    def send(self, value, *moves):
        key = self.add("send", value, tuple((a, b) for a, b, *_ in moves))
        for _, target, owner, first, count in moves:
            for chunk in range(first, first + count):
                self.arrived[target, owner, chunk] = (key, first, count)
        return key

    def four(self):
        half = CHUNKS // 2
        self.reach(0, 0)
        self.add("z", 0, 2, 0)
        self.add("turn")
        self.add("split")
        self.add("z", 0, 2, 1)
        self.add("stack", 0)
        self.reach(1, 0)
        self.add("swap", 0)
        self.add("z", 1, 2, 0)
        self.add("prepare", 0)
        zero, one, two, far = [], [], [], []
        for c in range(CHUNKS):
            zero.append(self.solve((0, c, 1)))
            self.send(zero[-1], (0, 1, 0, c, 1))
            if c == 0:
                self.reach("last", 0)
            if c == half - 1:
                far.append(self.send(self.join(*zero), (0, 2, 0, 0, half)))
                self.add("z", 1, 2, 1)
        far.append(self.send(self.join(*zero[half:]), (0, 2, 0, half, CHUNKS - half)))
        self.add("stack", 1)
        self.reach(2, 0)
        self.add("swap", 1)
        self.add("z", 2, 2, 0)
        self.add("prepare", 1)
        for c in range(CHUNKS):
            one.append(self.solve((1, c, 1)))
            self.send(one[-1], (1, 2, 1, c, 1))
            if c == 0:
                self.send(far[0], (2, 3, 0, 0, half))
                self.add("z", "last", 2, 0)
                self.add("z", 2, 2, 1)
            if c == half - 1:
                self.send(self.join(*one), (1, 3, 1, 0, half))
            if c == half:
                near = [self.arrived[1, 0, at][0] for at in range(half, CHUNKS)]
                self.send(self.join(*near), (1, 3, 0, half, CHUNKS - half))
                self.add("z", "last", 2, 1)
                self.pack(2)
        self.send(self.join(*one[half:]), (1, 3, 1, half, CHUNKS - half))
        for c in range(half):
            self.send(self.solve((2, c, 1)), (2, 3, 2, c, 1))
        self.pack("last")
        for c in range(half, CHUNKS):
            self.send(self.solve((2, c, 1)), (2, 3, 2, c, 1))
        early = self.solve((3, 0, half), only=(0, 1))
        self.solve((3, 0, half), base=early, done=(0, 1))
        late = [self.solve((3, c, 1), only=(0, 1)) for c in range(half, CHUNKS)]
        for c, base in zip(range(half, CHUNKS), late):
            self.solve((3, c, 1), base=base, done=(0, 1))

    def many(self):
        last, half = self.last, CHUNKS // 2
        self.add("turn")
        self.add("split")
        self.reach(0)
        self.reach(1)
        self.pack(0)
        for slot in range(CHUNKS + LAG * (last - 1)):
            d, extra = divmod(slot, LAG)
            if extra == 0 and 0 < d < last:
                if d == 1:
                    for far in range(2, last):
                        self.reach(far)
                self.pack(d)
            units = [(r, slot - LAG * r, 1) for r in range(last) if 0 <= slot - LAG * r < CHUNKS]
            key = self.solve(*units)
            for d in range(1, last):
                moves = [(r, r + d, r, c, 1) for r, c, _ in units if r + d < last or d == 1]
                if moves:
                    self.send(key, *moves)
            for r, c, _ in units:
                if r < last - 1 and (c + 1) % half == 0:
                    keys = [key for _, _, key in self.solved[r][-half:]]
                    self.send(self.join(*keys), (r, last, r, c + 1 - half, half))
        self.reach("last")
        self.pack("last")
        for first in (0, half):
            early = self.solve((last, first, half), only=range(last - 1))
            self.solve((last, first, half), base=early, done=range(last - 1))


def whole():
    return pl.BlockSpec(memory_space=pltpu.VMEM)


def body(plan, factor, inverses, right_side):
    return solve(plan, factor, inverses, right_side)


def solve(plan, factor, inverses, right_side):
    block, columns = right_side.shape
    per_block, panel, _ = inverses.shape
    rows, lanes, last = plan.rows, plan.lanes, plan.last
    row = lax.axis_index("row").astype(jnp.int32)
    lane = lax.axis_index("rhs").astype(jnp.int32)
    slices = jnp.transpose(factor, (1, 2, 0))
    width = slices.shape[1]
    piece = columns // CHUNKS
    scalar = pl.BlockSpec(memory_space=pltpu.SMEM)
    half = jax.ShapeDtypeStruct
    grant = pltpu.CompilerParams(vmem_limit_bytes=GRANT)
    where = row.reshape(1)

    def call(kernel, shapes, scalars, values):
        return pl.pallas_call(
            kernel, out_shape=shapes, in_specs=[scalar] * len(scalars) + [whole()] * len(values), compiler_params=grant
        )(*scalars, *values)

    def send(value, moves):
        pairs = [(a * lanes + b, c * lanes + d) for (a, b), (c, d) in moves]
        return lax.ppermute(value, ("row", "rhs"), pairs)

    def users(name):
        return [last] if name == "last" else range(name, rows if name == 0 else last)

    shared = {}
    masks = [0]
    for level in range(lanes.bit_length() - 2):
        masks += [mask ^ (lanes >> (level + 1)) for mask in masks]
    tiles = {}
    parts = {}
    for name in [*range(last), "last"]:
        if name == "last":
            own = slices[: last * per_block]
        elif name == 0:
            own = lax.dynamic_slice_in_dim(slices, row * per_block, per_block - 1, 0)[:, :, panel:]
        else:
            own = lax.dynamic_slice_in_dim(slices, jnp.maximum(row - name, 0) * per_block, per_block, 0)
        parts[name] = {0: own}
    stacked, swapped, values = {}, {}, {}

    def run(step):
        kind, *at = step
        if kind == "z":
            name, bit, index = at
            moves = [((r, q), (r, q ^ bit)) for r in users(name) for q in range(lanes)]
            parts[name][masks[index] ^ bit] = send(parts[name][masks[index]], moves)
        elif kind == "turn":
            values["residual"] = call(turn_kernel, half((columns, block), jnp.float32), [], [right_side])
        elif kind == "split":
            inv = call(split_kernel, [half(inverses.shape, jnp.bfloat16)] * 2, [], [inverses])
            shared.update(inv_high=inv[0], inv_low=inv[1])
        elif kind == "stack":
            mine = [parts[at[0]][mask] for mask in masks]
            shape = half((len(mine), *mine[0].shape), jnp.float32)
            stacked[at[0]] = call(stack_kernel, shape, [], mine)
        elif kind == "swap":
            moves = [((r, q), (r, q ^ 1)) for r in users(at[0]) for q in range(lanes)]
            swapped[at[0]] = send(stacked[at[0]], moves)
        elif kind == "prepare":
            name = at[0]
            mine = [parts[name][mask] for mask in masks]
            count, _, wide = mine[0].shape
            shape = half((count, width * lanes, wide), jnp.bfloat16)
            pair = call(functools.partial(prepare_kernel, masks), [shape] * 2, [lane.reshape(1)], [*mine, swapped[name]])
            for form, value in zip(("high", "low"), pair):
                if name == "last":
                    for g in range(last):
                        tiles["last", last - g, form] = value[g * per_block : (g + 1) * per_block].reshape(-1, wide)
                elif name == 0:
                    shared["own", form] = value.reshape(-1, wide)
                else:
                    tiles["near", name, form] = value.reshape(-1, wide)
        elif kind == "join":
            shape = half((sum(values[key].shape[0] for key in at), block), jnp.float32)
            values[step] = call(join_kernel, shape, [], [values[key] for key in at])
        elif kind == "send":
            key, pairs = at
            values[step] = send(values[key], [((a, q), (b, q)) for a, b in pairs for q in range(lanes)])
        elif kind == "solve":
            count, jobs, base, finish = at
            operands = dict(shared) if finish else {}
            if base is not None:
                operands[base] = values[base]
            layout = []
            for r, first, terms in jobs:
                made = []
                for spot, key, offset, length, distance in terms:
                    pair = ("last" if r == last else "near", distance)
                    operands[key] = values[key]
                    for form in ("high", "low"):
                        operands[pair + (form,)] = tiles[pair + (form,)]
                    made.append((spot * piece, key, offset * piece, length * piece, pair))
                layout.append((r, first * piece, base, made))
            values[step] = call(
                functools.partial(solve_kernel, (list(operands), layout, finish)),
                half((count * piece, block), jnp.float32),
                [where],
                [values["residual"], *operands.values()],
            )

    for step in plan.steps:
        run(step)

    keys = list(dict.fromkeys(key for parts in plan.solved.values() for _, _, key in parts))
    segments = [[(first * piece, count * piece, key) for first, count, key in plan.solved[r]] for r in range(rows)]
    return pl.pallas_call(
        functools.partial(place_kernel, keys, segments),
        out_shape=half((block, columns), jnp.float32),
        in_specs=[scalar] + [pl.BlockSpec(memory_space=pl.ANY)] * len(keys),
        scratch_shapes=[pltpu.VMEM((columns, block), jnp.float32), pltpu.SemaphoreType.DMA((CHUNKS,))],
        compiler_params=grant,
        name="place",
    )(where, *[values[key] for key in keys])


def solution(mesh):
    placed = (P("row", None, "rhs"), P("row", None, None), P("row", "rhs"))
    plan = Plan(mesh.shape["row"], mesh.shape["rhs"])
    return jax.shard_map(
        functools.partial(body, plan), mesh=mesh, in_specs=placed, out_specs=P("row", "rhs"), check_vma=False
    )
```

```python
import functools

import jax
import jax.numpy as jnp
from jax import lax
from jax.experimental import pallas as pl
from jax.experimental.pallas import tpu as pltpu
from jax.sharding import PartitionSpec as P


CHUNKS = 4
LAG = 2
GRANT = 12 * 1024 * 1024


def halves(value):
    high = value.astype(jnp.bfloat16)
    low = (value - high.astype(jnp.float32)).astype(jnp.bfloat16)
    return high, low


def times(left, high, low, contract=0):
    dims = (((1,), (contract,)), ((), ()))
    left_high, left_low = halves(left)
    dot = functools.partial(lax.dot_general, dimension_numbers=dims, preferred_element_type=jnp.float32)
    return dot(left_high, high) + (dot(left_low, high) + dot(left_high, low))


def below(count):
    return [(p, m) for p in range(count) for m in range(p + 1, count)]


def pick_kernel(per_block, where, slices, *outs):
    panel = outs[0].shape[2]
    for row, out in enumerate(outs):

        @pl.when(where[0] == row)
        def _():
            at = 0
            for p in range(row * per_block):
                for m in range(per_block):
                    out[at] = slices[p, :, m * panel : (m + 1) * panel]
                    at += 1
            for p, m in below(per_block):
                out[at] = slices[row * per_block + p, :, m * panel : (m + 1) * panel]
                at += 1


def prepare_kernel(masks, per_block, row, where, place, *refs):
    parts, (swapped, *outs) = refs[: len(masks)], refs[len(masks) :]
    _, total, width, panel = swapped.shape
    near = row * per_block * per_block
    own = outs[-2:]

    @pl.when(where[0] == row)
    def _():
        for step, (mask, part) in enumerate(zip(masks, parts)):
            source = place[0] ^ mask
            for spot, value in ((source, part), (source ^ 1, swapped.at[step])):
                spot = pl.multiple_of(spot * width, width)
                for p in range(row * per_block):
                    for m in range(per_block):
                        first, second = halves(value[p * per_block + m])
                        outs[0][p, pl.ds(spot, width), m * panel : (m + 1) * panel] = first
                        outs[1][p, pl.ds(spot, width), m * panel : (m + 1) * panel] = second
                first, second = halves(value[near:total])
                own[0][:, pl.ds(spot, width), :] = first
                own[1][:, pl.ds(spot, width), :] = second


def turn_kernel(value, out):
    out[...] = value[...].T


def split_kernel(value, high, low):
    high[...], low[...] = halves(value[...])


def solve_into(out, inv_high, inv_low, own_high, own_low):
    count, panel, _ = inv_high.shape
    spots = [slice(p * panel, (p + 1) * panel) for p in range(count)]
    for p in range(count):
        solved = times(out[:, spots[p]], inv_high[p], inv_low[p], 1)
        out[:, spots[p]] = solved
        for tile, (source, m) in enumerate(below(count)):
            if source == p:
                out[:, spots[m]] -= times(solved, own_high[tile], own_low[tile])


def solve_kernel(layout, place, residual, *refs):
    *inputs, out = refs
    names, jobs, finish = layout
    at = dict(zip(names, inputs))
    rows, block = out.shape
    for row, first, base, terms in jobs:

        @pl.when(place[0] == row)
        def _():
            out[...] = residual[first : first + rows, :] if base is None else at[base][...]
            for spot, key, offset, length, owner in terms:
                here = slice(spot, spot + length)
                tiles = slice(owner * block, (owner + 1) * block)
                solved = at[key][offset : offset + length, :]
                out[here, :] -= times(solved, at[row, "high"][tiles, :], at[row, "low"][tiles, :])
            if finish:
                solve_into(out, at["inv_high"], at["inv_low"], at[row, "own_high"], at[row, "own_low"])


def stack_kernel(row, where, *refs):
    *inputs, out = refs

    @pl.when(where[0] == row)
    def _():
        for step, value in enumerate(inputs):
            out[step] = value[...]


def join_kernel(*refs):
    *inputs, out = refs
    rows = inputs[0].shape[0]
    for step, value in enumerate(inputs):
        out[step * rows : (step + 1) * rows, :] = value[...]


def place_kernel(names, segments, place, *refs):
    *inputs, out, stage, sems = refs
    at = dict(zip(names, inputs))
    for row, parts in enumerate(segments):

        @pl.when(place[0] == row)
        def _():
            copies = []
            for step, (first, length, key) in enumerate(parts):
                copies.append(pltpu.make_async_copy(at[key], stage.at[pl.ds(first, length)], sems.at[step]))
                copies[-1].start()
            for copy in copies:
                copy.wait()

    out[...] = stage[...].T


class Plan:
    def __init__(self, rows, lanes):
        self.rows, self.lanes, self.last = rows, lanes, rows - 1
        self.steps = []
        self.arrived = {}
        self.solved = {row: [] for row in range(rows)}
        if rows == 4:
            self.four()
        else:
            self.many()

    def add(self, *step):
        if step not in self.steps:
            self.steps.append(step)
        return step

    def reach(self, name, *levels):
        count = self.lanes.bit_length() - 2
        for level in levels or range(count):
            bit = self.lanes >> (level + 1)
            for index in range(1 << level):
                self.add("z", name, bit, index)

    def pack(self, name):
        for kind in ("stack", "swap", "prepare"):
            self.add(kind, name)

    def solve(self, *units, base=None, done=(), only=None):
        jobs = []
        for row, first, count in units:
            owners = range(row) if only is None else only
            terms = []
            for owner in owners:
                if owner in done:
                    continue
                chunk = first
                while chunk < first + count:
                    key, start, length = self.arrived[row, owner, chunk]
                    length = min(length - (chunk - start), first + count - chunk)
                    terms.append((chunk - first, key, chunk - start, length, owner))
                    chunk += length
            jobs.append((row, first, tuple(terms)))
        key = self.add("solve", units[0][2], tuple(jobs), base, only is None)
        if only is None:
            for row, first, count in units:
                self.solved[row].append((first, count, key))
        return key

    def join(self, *keys):
        return self.add("join", *keys)

    def send(self, value, *moves):
        key = self.add("send", value, tuple((a, b) for a, b, *_ in moves))
        for _, target, owner, first, count in moves:
            for chunk in range(first, first + count):
                self.arrived[target, owner, chunk] = (key, first, count)
        return key

    def four(self):
        half = CHUNKS // 2
        zero, one = [], []

        def first(c):
            zero.append(self.solve((0, c, 1)))
            self.send(zero[-1], (0, 1, 0, c, 1))

        def second(c):
            one.append(self.solve((1, c, 1)))
            self.send(one[-1], (1, 2, 1, c, 1))

        def third(c):
            self.send(self.solve((2, c, 1)), (2, 3, 2, c, 1))

        def pass_on(c):
            self.send(self.arrived[1, 0, c][0], (1, 3, 0, c, 1))

        def relay(c):
            self.send(self.arrived[3, 0, c][0], (3, 2, 0, c, 1))

        self.add("z", 0, 4, 0)
        self.add("z", 0, 2, 0)
        self.add("z", 1, 4, 0)
        self.add("z", 0, 2, 1)
        self.add("z", 2, 4, 0)
        self.add("z", 3, 4, 0)
        self.add("stack", 0)
        self.add("swap", 0)
        self.add("turn")
        self.add("split")
        self.add("z", 1, 2, 0)
        self.add("prepare", 0)
        first(0)
        first(1)
        self.add("z", 1, 2, 1)
        self.add("z", 2, 2, 0)
        self.add("z", 3, 2, 0)
        for c in range(half):
            self.send(zero[c], (0, 2, 0, c, 1))
        for c in range(half, CHUNKS):
            first(c)
        self.add("stack", 1)
        self.add("swap", 1)
        pass_on(0)
        self.add("prepare", 1)
        self.add("z", 2, 2, 1)
        second(0)
        second(1)
        pass_on(half)
        self.add("z", 3, 2, 1)
        self.send(self.arrived[2, 0, 1][0], (2, 3, 0, 1, 1))
        pass_on(half + 1)
        self.send(self.join(*one), (1, 3, 1, 0, half))
        relay(half)
        second(half)
        self.send(one[half], (1, 3, 1, half, 1))
        self.pack(2)
        third(0)
        second(half + 1)
        relay(half + 1)
        third(1)
        self.send(one[half + 1], (1, 3, 1, half + 1, 1))
        third(half)
        self.add("stack", 3)
        self.add("swap", 3)
        third(half + 1)
        self.add("prepare", 3)
        early = self.solve((3, 0, half), only=(0, 1))
        self.solve((3, 0, half), base=early, done=(0, 1))
        for c in range(half, CHUNKS):
            base = self.solve((3, c, 1), only=(0, 1))
            self.solve((3, c, 1), base=base, done=(0, 1))

    def many(self):
        last, half = self.last, CHUNKS // 2
        self.add("turn")
        self.add("split")
        self.reach(0)
        for slot in range(CHUNKS + LAG * (last - 1)):
            d, extra = divmod(slot, LAG)
            if extra == 0 and d < last:
                self.pack(d)
                self.reach(d + 1)
            units = [(r, slot - LAG * r, 1) for r in range(last) if 0 <= slot - LAG * r < CHUNKS]
            key = self.solve(*units)
            for d in range(1, last):
                moves = [(r, r + d, r, c, 1) for r, c, _ in units if r + d < last or d == 1]
                if moves:
                    self.send(key, *moves)
            for r, c, _ in units:
                if r < last - 1 and (c + 1) % half == 0:
                    keys = [key for _, _, key in self.solved[r][-half:]]
                    self.send(self.join(*keys), (r, last, r, c + 1 - half, half))
        self.pack(last)
        for first in (0, half):
            early = self.solve((last, first, half), only=range(last - 1))
            self.solve((last, first, half), base=early, done=range(last - 1))


def whole():
    return pl.BlockSpec(memory_space=pltpu.VMEM)


def body(plan, factor, inverses, right_side):
    return solve(plan, factor, inverses, right_side)


def solve(plan, factor, inverses, right_side):
    block, columns = right_side.shape
    per_block, panel, _ = inverses.shape
    rows, lanes = plan.rows, plan.lanes
    row = lax.axis_index("row").astype(jnp.int32)
    lane = lax.axis_index("rhs").astype(jnp.int32)
    slices = jnp.transpose(factor, (1, 2, 0))
    width = slices.shape[1]
    piece = columns // CHUNKS
    scalar = pl.BlockSpec(memory_space=pltpu.SMEM)
    half = jax.ShapeDtypeStruct
    grant = pltpu.CompilerParams(vmem_limit_bytes=GRANT)
    where = row.reshape(1)

    def call(kernel, shapes, scalars, values):
        return pl.pallas_call(
            kernel, out_shape=shapes, in_specs=[scalar] * len(scalars) + [whole()] * len(values), compiler_params=grant
        )(*scalars, *values)

    def send(value, moves):
        pairs = [(a * lanes + b, c * lanes + d) for (a, b), (c, d) in moves]
        return lax.ppermute(value, ("row", "rhs"), pairs)

    shared = {}
    masks = [0]
    for level in range(lanes.bit_length() - 2):
        masks += [mask ^ (lanes >> (level + 1)) for mask in masks]
    tiles = {}
    triangle = len(below(per_block))
    sizes = [r * per_block * per_block + triangle for r in range(rows)]
    picked = call(
        functools.partial(pick_kernel, per_block),
        [half((size, width, panel), jnp.float32) for size in sizes],
        [where],
        [slices],
    )
    parts = [{0: value} for value in picked]
    stacked, swapped, values = {}, {}, {}

    def run(step):
        kind, *at = step
        if kind == "z":
            name, bit, index = at
            moves = [((name, q), (name, q ^ bit)) for q in range(lanes)]
            parts[name][masks[index] ^ bit] = send(parts[name][masks[index]], moves)
        elif kind == "turn":
            values["residual"] = call(turn_kernel, half((columns, block), jnp.float32), [], [right_side])
        elif kind == "split":
            inv = call(split_kernel, [half(inverses.shape, jnp.bfloat16)] * 2, [], [inverses])
            shared.update(inv_high=inv[0], inv_low=inv[1])
        elif kind == "stack":
            mine = [parts[at[0]][mask] for mask in masks]
            shape = half((len(mine), *mine[0].shape), jnp.float32)
            stacked[at[0]] = call(functools.partial(stack_kernel, at[0]), shape, [where], mine)
        elif kind == "swap":
            moves = [((at[0], q), (at[0], q ^ 1)) for q in range(lanes)]
            swapped[at[0]] = send(stacked[at[0]], moves)
        elif kind == "prepare":
            name = at[0]
            mine = [parts[name][mask] for mask in masks]
            shapes = [half((triangle, panel, panel), jnp.bfloat16)] * 2
            if name:
                shapes = [half((name * per_block, panel, block), jnp.bfloat16)] * 2 + shapes
            made = call(
                functools.partial(prepare_kernel, masks, per_block, name),
                shapes,
                [where, lane.reshape(1)],
                [*mine, swapped[name]],
            )
            tiles[name, "own_high"], tiles[name, "own_low"] = made[-2:]
            if name:
                tiles[name, "high"], tiles[name, "low"] = [value.reshape(-1, block) for value in made[:2]]
        elif kind == "join":
            shape = half((sum(values[key].shape[0] for key in at), block), jnp.float32)
            values[step] = call(join_kernel, shape, [], [values[key] for key in at])
        elif kind == "send":
            key, pairs = at
            values[step] = send(values[key], [((a, q), (b, q)) for a, b in pairs for q in range(lanes)])
        elif kind == "solve":
            count, jobs, base, finish = at
            operands = dict(shared) if finish else {}
            if base is not None:
                operands[base] = values[base]
            layout = []
            for r, first, terms in jobs:
                made = []
                forms = ["own_high", "own_low"] if finish else []
                forms += ["high", "low"] if terms else []
                for form in forms:
                    operands[r, form] = tiles[r, form]
                for spot, key, offset, length, owner in terms:
                    operands[key] = values[key]
                    made.append((spot * piece, key, offset * piece, length * piece, owner))
                layout.append((r, first * piece, base, made))
            values[step] = call(
                functools.partial(solve_kernel, (list(operands), layout, finish)),
                half((count * piece, block), jnp.float32),
                [where],
                [values["residual"], *operands.values()],
            )

    for step in plan.steps:
        run(step)

    keys = list(dict.fromkeys(key for parts in plan.solved.values() for _, _, key in parts))
    segments = [[(first * piece, count * piece, key) for first, count, key in plan.solved[r]] for r in range(rows)]
    return pl.pallas_call(
        functools.partial(place_kernel, keys, segments),
        out_shape=half((block, columns), jnp.float32),
        in_specs=[scalar] + [pl.BlockSpec(memory_space=pl.ANY)] * len(keys),
        scratch_shapes=[pltpu.VMEM((columns, block), jnp.float32), pltpu.SemaphoreType.DMA((CHUNKS,))],
        compiler_params=grant,
        name="place",
    )(where, *[values[key] for key in keys])


def solution(mesh):
    placed = (P("row", None, "rhs"), P("row", None, None), P("row", "rhs"))
    plan = Plan(mesh.shape["row"], mesh.shape["rhs"])
    return jax.shard_map(
        functools.partial(body, plan), mesh=mesh, in_specs=placed, out_specs=P("row", "rhs"), check_vma=False
    )
```
